16 devices in a mesh: rep: 1, dp: 16 (over x, y, z, core).
Axes of the slice: x: 2, y: 2, z: 2, core: 2. Of those that a mesh axis runs over, the one named last changes fastest.
Arguments:
- g_w_gate: bfloat16 [16, 2, 1280, 4480], P(('rep', 'dp'))
- g_w_up: bfloat16 [16, 2, 1280, 4480], P(('rep', 'dp'))
- g_w_down: bfloat16 [16, 2, 4480, 1280], P(('rep', 'dp'))
- w_gate: bfloat16 [2, 1280, 4480], replicated
- w_up: bfloat16 [2, 1280, 4480], replicated
- w_down: bfloat16 [2, 4480, 1280], replicated
- m_w_gate: float32 [2, 1280, 4480], P(None, 'dp')
- m_w_up: float32 [2, 1280, 4480], P(None, 'dp')
- m_w_down: float32 [2, 4480, 1280], P(None, 'dp')
- v_w_gate: float32 [2, 1280, 4480], P(None, 'dp')
- v_w_up: float32 [2, 1280, 4480], P(None, 'dp')
- v_w_down: float32 [2, 4480, 1280], P(None, 'dp')
Outputs:
- output 1: bfloat16 [2, 1280, 4480], P('rep')
- output 2: bfloat16 [2, 1280, 4480], P('rep')
- output 3: bfloat16 [2, 4480, 1280], P('rep')
- output 4: float32 [2, 1280, 4480], P('rep', 'dp')
- output 5: float32 [2, 1280, 4480], P('rep', 'dp')
- output 6: float32 [2, 4480, 1280], P('rep', 'dp')
- output 7: float32 [2, 1280, 4480], P('rep', 'dp')
- output 8: float32 [2, 1280, 4480], P('rep', 'dp')
- output 9: float32 [2, 4480, 1280], P('rep', 'dp')
All inputs are finite; a program needn't handle non-finite values.
Results may differ from the reference program's by a relative error of at most 0.022.
Values are sent between devices in bfloat16 or wider.
A program may use at most 2 GiB of HBM per device.

```python
import jax
import jax.numpy as jnp
from jax import lax

DEVICES = 16
D = 1280
FF = 4480
LAYERS = 2
NAMES = ("w_gate", "w_up", "w_down")
SHAPES = {"w_gate": (LAYERS, D, FF), "w_up": (LAYERS, D, FF), "w_down": (LAYERS, FF, D)}


def setup_inputs(seed: int = 0, part: int = 0) -> dict:
    kz, *keys = jax.random.split(jax.random.key(seed), 1 + 5 * len(NAMES))
    loud = 2.0 ** jax.random.uniform(kz, (), jnp.float32, -1.0, 1.0)
    drawn = {}
    for name, key, both in zip(NAMES, keys[:3], keys[3:6], strict=True):
        own = jax.random.normal(jax.random.fold_in(key, part), (DEVICES, *SHAPES[name]), jnp.float32)
        shared = jax.random.normal(jax.random.fold_in(both, part), SHAPES[name], jnp.float32)
        drawn["g_" + name] = (loud * (0.7 * shared / DEVICES + 0.7 * own * DEVICES**-0.5)).astype(jnp.bfloat16)
    for name, key in zip(NAMES, keys[6:9], strict=True):
        drawn[name] = (jax.random.normal(key, SHAPES[name], jnp.float32) * SHAPES[name][1] ** -0.5).astype(jnp.bfloat16)
    for name, key in zip(NAMES, keys[9:12], strict=True):
        drawn["m_" + name] = loud * 0.5 * jax.random.normal(key, SHAPES[name], jnp.float32)
    for name, key in zip(NAMES, keys[12:15], strict=True):
        drawn["v_" + name] = loud * loud * jax.random.uniform(key, SHAPES[name], jnp.float32, 0.5, 1.5)
    return drawn


def adamw(w, m, v, g):
    m = 0.9 * m + 0.1 * g
    v = 0.95 * v + 0.05 * g * g
    step = m * lax.rsqrt(v + 1e-8) + 0.1 * w
    return (w - 0.02 * step).astype(jnp.bfloat16), m, v


def reference(g_w_gate, g_w_up, g_w_down, w_gate, w_up, w_down, m_w_gate, m_w_up, m_w_down, v_w_gate, v_w_up, v_w_down):
    def total(terms):
        return lax.scan(lambda so_far, term: (so_far + term.astype(jnp.float32), None), jnp.zeros(terms.shape[1:], jnp.float32), terms)[0]

    gradients = [total(terms).astype(jnp.bfloat16).astype(jnp.float32) for terms in (g_w_gate, g_w_up, g_w_down)]
    new = [
        adamw(w.astype(jnp.float32), m, v, g)
        for w, m, v, g in zip((w_gate, w_up, w_down), (m_w_gate, m_w_up, m_w_down), (v_w_gate, v_w_up, v_w_down), gradients, strict=True)
    ]
    return tuple(one[which] for which in range(3) for one in new)
```

```python
import jax
import jax.numpy as jnp
from jax import lax
from jax.experimental import pallas as pl
from jax.experimental.pallas import tpu as pltpu
from jax.sharding import PartitionSpec as P

MESH = pl.DeviceIdType.MESH
BITS = (4, 2, 1)
AXES = 3


def order(stream):
    return tuple(BITS[(stream + i) % AXES] for i in range(AXES))


def halving(stream):
    a, b, c = order(stream)
    return {1: (a | b | c, a | b, a | c, a), 2: (b | c, b), 3: (c,), 4: (0,)}


def inputs_of(stream, step, r):
    a, b, c = order(stream)
    sub = (0, c, b, b | c)
    slots = [r]
    if step >= 2:
        slots.append(8 + sub.index(r))
    if step >= 3:
        slots.append(12 + (0, c).index(r))
    if step >= 4:
        slots.append(14)
    return slots


def lands_at(stream, step, r):
    a, b, c = order(stream)
    if step == 1:
        return 8 + (0, c, b, b | c).index(r ^ a)
    if step == 2:
        return 12 + (0, c).index(r ^ b)
    return 14


def plan():
    rs = lambda m, step, i: ("rs", m, step, i)
    ag = lambda m, axis, i: ("ag", m, axis, i)
    return (
        [rs(0, 1, i) for i in range(4)]
        + [rs(1, 1, 0), rs(0, 2, 0), rs(1, 1, 1), rs(0, 2, 1), rs(1, 1, 2)]
        + [rs(0, 3, 0), rs(1, 1, 3), rs(1, 2, 0), rs(1, 2, 1), rs(0, 4, 0)]
        + [ag(0, 0, 0), ag(0, 1, 0), ag(0, 2, 0), rs(1, 3, 0)]
        + [ag(0, 1, 1), ag(0, 2, 1), ag(0, 2, 2), ("c", 0, 0), rs(1, 4, 0)]
        + [ag(1, 0, 0), ag(1, 1, 0), ag(1, 2, 0), ag(0, 2, 3), ("c", 0, 1), ("c", 0, 2)]
        + [ag(1, 1, 1), ag(1, 2, 1), ("c", 1, 0), ag(1, 2, 2), ("c", 0, 3), ag(1, 2, 3)]
        + [("c", 1, 1), ("c", 1, 2), ("c", 1, 3)]
    )


AHEAD = 4


def kernel(*refs):
    g, w, m_in, v_in = (refs[i : i + 3] for i in (0, 3, 6, 9))
    out, m_out, v_out, land = (refs[i : i + 3] for i in (12, 15, 18, 21))
    stage, sent, m_buf, v_buf, w_buf, new = (refs[i : i + 3] for i in (24, 27, 30, 33, 36, 39))
    load_sem, state_sem, store_sem, cs_sem, cr_sem, rs_sem, rr_sem, as_sem, ar_sem, ds_sem, dr_sem = refs[42:]

    me = lax.axis_index("dp")
    chip, core = me // 2, me % 2
    partner = chip * 2 + (1 - core)

    def flip(bits):
        at = chip
        for bit in BITS:
            if bits & bit:
                at = at + bit - 2 * bit * ((at // bit) % 2)
        return at

    near = {bit: flip(bit) * 2 + core for bit in BITS}
    near[0] = partner

    barrier = pltpu.get_barrier_semaphore()
    for other in near.values():
        pl.semaphore_signal(barrier, inc=1, device_id={"dp": other}, device_id_type=MESH)
    pl.semaphore_wait(barrier, len(near))

    rows = [x.shape[1] for x in m_in]

    def block(s, r, of):
        return pl.ds(pl.multiple_of((flip(r) * 2 + of) * rows[s], 8), rows[s])

    def remote(src, dst, send, recv, to):
        return pltpu.make_async_remote_copy(
            src_ref=src, dst_ref=dst, send_sem=send, recv_sem=recv, device_id={"dp": to}, device_id_type=MESH
        )

    def cross(s, m, r):
        i = (s * 2 + m) * 8 + r
        return remote(g[s].at[0, m, block(s, r, 1 - core)], land[s].at[m, r], cs_sem.at[i], cr_sem.at[i], partner)

    def fall(s, m, step, r):
        slot = lands_at(s, step, r)
        i = (s * 2 + m) * 7 + slot - 8
        return remote(sent[s].at[m, slot - 8], land[s].at[m, slot], rs_sem.at[i], rr_sem.at[i], near[order(s)[step - 1]])

    def rise(s, m, axis, i):
        turn = order(s)
        known = (0, turn[0], turn[1], turn[0] | turn[1])[i]
        r = known | turn[axis]
        at = (s * 2 + m) * 7 + r - 1
        rows_of = block(s, known, core)
        src = new[s].at[m] if known == 0 else out[s].at[m, rows_of]
        return known, r, remote(src, out[s].at[m, rows_of], as_sem.at[at], ar_sem.at[at], near[turn[axis]])

    def over(s, m, r):
        i = (s * 2 + m) * 8 + r
        rows_of = block(s, r, core)
        src = new[s].at[m] if r == 0 else out[s].at[m, rows_of]
        return remote(src, out[s].at[m, rows_of], ds_sem.at[i], dr_sem.at[i], partner)

    def arrived(s, m, r):
        turn = order(s)
        last = max(axis for axis in range(AXES) if r & turn[axis])
        i = (0, turn[0], turn[1], turn[0] | turn[1]).index(r ^ turn[last])
        rise(s, m, last, i)[2].wait_recv()
        over(s, m, r).start()

    def state(s, m):
        pairs = ((m_in[s].at[m], m_buf[s]), (v_in[s].at[m], v_buf[s]), (w[s].at[m, block(s, 0, core)], w_buf[s]))
        return [pltpu.make_async_copy(src, dst, state_sem.at[s * 3 + i]) for i, (src, dst) in enumerate(pairs)]

    def store(s, m):
        pairs = ((m_buf[s], m_out[s].at[m]), (v_buf[s], v_out[s].at[m]), (new[s].at[m], out[s].at[m, block(s, 0, core)]))
        return [pltpu.make_async_copy(src, dst, store_sem.at[s * 3 + i]) for i, (src, dst) in enumerate(pairs)]

    def chunks(s, body):
        whole = rows[s] // 16

        @pl.loop(0, whole)
        def _(i):
            body(pl.ds(pl.multiple_of(i * 16, 16), 16))

        if rows[s] % 16:
            body(pl.ds(whole * 16, rows[s] % 16))

    def total(s, n, at):
        so_far = stage[s][0, at, :].astype(jnp.float32)
        for i in range(1, n):
            so_far = so_far + stage[s][i, at, :].astype(jnp.float32)
        return so_far

    def add(s, m, step, r, n):
        slot = lands_at(s, step, r) - 8

        def body(at):
            sent[s][m, slot, at, :] = total(s, n, at).astype(jnp.bfloat16)

        chunks(s, body)

    def adamw(s, m, n):
        def body(at):
            gradient = total(s, n, at).astype(jnp.bfloat16).astype(jnp.float32)
            w_old = w_buf[s][at, :].astype(jnp.float32)
            m_new = 0.9 * m_buf[s][at, :] + 0.1 * gradient
            v_new = 0.95 * v_buf[s][at, :] + 0.05 * gradient * gradient
            step = m_new * lax.rsqrt(v_new + 1e-8) + 0.1 * w_old
            m_buf[s][at, :] = m_new
            v_buf[s][at, :] = v_new
            new[s][m, at, :] = (w_old - 0.02 * step).astype(jnp.bfloat16)

        chunks(s, body)

    todo = plan()
    sums = [entry for entry in todo if entry[0] == "rs"]

    def send_cross(entry):
        _, m, step, i = entry
        for s in range(AXES):
            cross(s, m, halving(s)[step][i]).start()

    for entry in sums[:AHEAD]:
        send_cross(entry)
    for s in range(AXES):
        for copy in state(s, 0):
            copy.start()
    done = 0
    for entry in todo:
        if entry[0] == "rs":
            _, m, step, i = entry
            if done + AHEAD < len(sums):
                send_cross(sums[done + AHEAD])
            done += 1
            loads = []
            for s in range(AXES):
                r = halving(s)[step][i]
                slots = inputs_of(s, step, r)
                copies = [pltpu.make_async_copy(g[s].at[0, m, block(s, r, core)], stage[s].at[0], load_sem.at[s * 5])]
                for k, slot in enumerate(slots):
                    if slot < 8:
                        cross(s, m, slot).wait_recv()
                    else:
                        before = 1 if slot < 12 else 2 if slot < 14 else 3
                        turned = next(x for x in halving(s)[before] if lands_at(s, before, x) == slot)
                        fall(s, m, before, turned).wait_recv()
                    copies.append(pltpu.make_async_copy(land[s].at[m, slot], stage[s].at[k + 1], load_sem.at[s * 5 + k + 1]))
                for copy in copies:
                    copy.start()
                loads.append(copies)
            for s in range(AXES):
                r = halving(s)[step][i]
                for copy in loads[s]:
                    copy.wait()
                if step < 4:
                    add(s, m, step, r, len(loads[s]))
                    fall(s, m, step, r).start()
                else:
                    for copy in state(s, m):
                        copy.wait()
                    adamw(s, m, len(loads[s]))
                    over(s, m, 0).start()
                    for copy in store(s, m):
                        copy.start()
        elif entry[0] == "ag":
            _, m, axis, i = entry
            for s in range(AXES):
                known, _, copy = rise(s, m, axis, i)
                if i and axis == (1 if i == 1 else 2):
                    arrived(s, m, known)
                copy.start()
            if (m, axis, i) == (0, 2, 0):
                for s in range(AXES):
                    for copy in store(s, 0):
                        copy.wait()
                    for copy in state(s, 1):
                        copy.start()
        else:
            _, m, i = entry
            for s in range(AXES):
                turn = order(s)
                arrived(s, m, (0, turn[0], turn[1], turn[0] | turn[1])[i] | turn[2])

    for s in range(AXES):
        for copy in store(s, 1):
            copy.wait()
    for m in range(2):
        for s in range(AXES):
            for r in range(8):
                over(s, m, r).wait_recv()
                over(s, m, r).wait_send()
                cross(s, m, r).wait_send()
            for step in (1, 2, 3):
                for r in halving(s)[step]:
                    fall(s, m, step, r).wait_send()
            for axis in range(AXES):
                for i in range(2**axis):
                    rise(s, m, axis, i)[2].wait_send()


def solution(mesh):
    def step(*arrays):
        g, w, m, v = (arrays[i : i + 3] for i in (0, 3, 6, 9))
        layers = m[0].shape[0]
        blocks = [one.shape[1:] for one in m]
        shapes = (
            [jax.ShapeDtypeStruct(x.shape, x.dtype) for x in (*w, *m, *v)]
            + [jax.ShapeDtypeStruct((layers, 15, *b), jnp.bfloat16) for b in blocks]
        )
        anywhere = pl.BlockSpec(memory_space=pl.ANY)
        dma = pltpu.SemaphoreType.DMA
        result = pl.pallas_call(
            kernel,
            out_shape=shapes,
            in_specs=[anywhere] * 12,
            out_specs=[anywhere] * len(shapes),
            scratch_shapes=[
                *(pltpu.VMEM((5, *b), jnp.bfloat16) for b in blocks),
                *(pltpu.VMEM((layers, 7, *b), jnp.bfloat16) for b in blocks),
                *(pltpu.VMEM(b, jnp.float32) for b in blocks),
                *(pltpu.VMEM(b, jnp.float32) for b in blocks),
                *(pltpu.VMEM(b, jnp.bfloat16) for b in blocks),
                *(pltpu.VMEM((layers, *b), jnp.bfloat16) for b in blocks),
                dma((15,)),
                dma((9,)),
                dma((9,)),
                dma((48,)),
                dma((48,)),
                dma((42,)),
                dma((42,)),
                dma((42,)),
                dma((42,)),
                dma((48,)),
                dma((48,)),
            ],
            compiler_params=pltpu.CompilerParams(collective_id=0, has_side_effects=True, vmem_limit_bytes=67_000_000),
            name="sum_step_gather",
        )(*g, *w, *m, *v)
        return tuple(result[:9])

    all_of, cut = P(None, None, None), P(None, "dp", None)
    return jax.shard_map(
        step,
        mesh=mesh,
        in_specs=(P(("rep", "dp"), None, None, None),) * 3 + (all_of,) * 3 + (cut,) * 6,
        out_specs=(P("rep", None, None),) * 3 + (P("rep", "dp", None),) * 6,
        check_vma=False,
    )
```
